8 devices in a mesh: dp: 2 (over z, y), ep: 4 (over x, core).
Axes of the slice: x: 2, y: 2, z: 1, core: 2. Of those that a mesh axis runs over, the one named last changes fastest.
Arguments:
- x: bfloat16 [16384, 768], P(('dp', 'ep'))
- gy: bfloat16 [16384, 768], P(('dp', 'ep'))
- idx: int32 [16384], P(('dp', 'ep'))
- w_gate: bfloat16 [768, 8], replicated
- w_up: bfloat16 [8, 768, 3072], P('ep')
- w_down: bfloat16 [8, 3072, 768], P('ep')
Outputs:
- output 1: bfloat16 [16384, 768], P(('dp', 'ep'))
- output 2: bfloat16 [16384, 768], P(('dp', 'ep'))
- output 3: float32 [8, 768, 3072], P('ep')
- output 4: float32 [8, 3072, 768], P('ep')
- output 5: float32 [768, 8], replicated
All inputs are finite; a program needn't handle non-finite values.
Results may differ from the reference program's by a relative error of at most 0.00593475.
Values are sent between devices in bfloat16 or wider.
A program may use at most 1 GiB of HBM per device.

```python
import functools
import jax
import jax.numpy as jnp
from jax import lax

D_MODEL = 768
D_FF = 3072
N_EXPERTS = 8
TOKENS_DEV = 2048
N_DEVICES = 8
TILE_ROWS = 128
N_TOKENS = N_DEVICES * TOKENS_DEV
CAP_ROWS = 4 * TOKENS_DEV // N_EXPERTS
N_TILES = N_TOKENS // TILE_ROWS + N_EXPERTS


def count_profile():
    hot_experts = max(1, N_EXPERTS // 16)
    cold_experts = N_EXPERTS - hot_experts
    rest_rows = TOKENS_DEV - hot_experts * CAP_ROWS
    base_rows = rest_rows // cold_experts
    extra_rows = rest_rows % cold_experts
    return [CAP_ROWS] * hot_experts + [base_rows + 1] * extra_rows + [base_rows] * (cold_experts - extra_rows)


def draw_routing(route_key):
    profile = count_profile()
    rank_table = jnp.array([rank_id for rank_id in range(N_EXPERTS) for copy_num in range(profile[rank_id])], jnp.int32)

    def one_device(dev_key):
        perm_key, shuffle_key = jax.random.split(dev_key)
        expert_perm = jax.random.permutation(perm_key, N_EXPERTS).astype(jnp.int32)
        return jax.random.permutation(shuffle_key, expert_perm[rank_table])

    return jax.vmap(one_device)(jax.random.split(route_key, N_DEVICES)).reshape(N_TOKENS)


def setup_inputs(seed: int = 0) -> dict:
    root_key = jax.random.key(seed)
    k_x, k_gy, k_gate, k_up, k_down, k_route = jax.random.split(root_key, 6)
    x = jax.random.normal(k_x, (N_TOKENS, D_MODEL), jnp.float32).astype(jnp.bfloat16)
    gy = jax.random.normal(k_gy, (N_TOKENS, D_MODEL), jnp.float32).astype(jnp.bfloat16)
    w_gate = (jax.random.normal(k_gate, (D_MODEL, N_EXPERTS), jnp.float32) * D_MODEL ** -0.5).astype(jnp.bfloat16)
    w_up = (jax.random.normal(k_up, (N_EXPERTS, D_MODEL, D_FF), jnp.float32) * D_MODEL ** -0.5).astype(jnp.bfloat16)
    w_down = (jax.random.normal(k_down, (N_EXPERTS, D_FF, D_MODEL), jnp.float32) * D_FF ** -0.5).astype(jnp.bfloat16)
    idx = draw_routing(k_route)
    return {'x': x, 'gy': gy, 'idx': idx, 'w_gate': w_gate, 'w_up': w_up, 'w_down': w_down}


def tile_pass(w_up, w_down, grad_carry, tile_in):
    grad_up, grad_down = grad_carry
    tok_rows, d_out, expert = tile_in
    up_mat = w_up[expert]
    down_mat = w_down[expert]
    pre_act = jnp.dot(tok_rows, up_mat, preferred_element_type=jnp.float32)
    hid_full, gelu_back = jax.vjp(jax.nn.gelu, pre_act)
    hidden = hid_full.astype(jnp.bfloat16)
    y_rows = jnp.dot(hidden, down_mat, preferred_element_type=jnp.float32).astype(jnp.bfloat16)
    d_hidden = jnp.dot(d_out, down_mat.T, preferred_element_type=jnp.float32)
    d_pre = gelu_back(d_hidden)[0].astype(jnp.bfloat16)
    grad_down = grad_down.at[expert].add(jnp.dot(hidden.T, d_out, preferred_element_type=jnp.float32))
    grad_up = grad_up.at[expert].add(jnp.dot(tok_rows.T, d_pre, preferred_element_type=jnp.float32))
    d_rows = jnp.dot(d_pre, up_mat.T, preferred_element_type=jnp.float32).astype(jnp.bfloat16)
    return (grad_up, grad_down), (y_rows, d_rows)


def reference(x, gy, idx, w_gate, w_up, w_down):
    onehot = idx[:, None] == jnp.arange(N_EXPERTS, dtype=jnp.int32)[None, :]
    router_logit = jnp.dot(x, w_gate, preferred_element_type=jnp.float32)
    router_prob = jax.nn.softmax(router_logit, axis=-1)
    gate_val = N_EXPERTS * jnp.sum(jnp.where(onehot, router_prob, 0.0), axis=1)
    expert_count = jnp.sum(onehot, axis=0, dtype=jnp.int32)
    sort_order = jnp.argsort(idx, stable=True)
    sorted_pos = jnp.argsort(sort_order)
    expert_start = jnp.cumsum(expert_count) - expert_count
    tile_count = (expert_count + TILE_ROWS - 1) // TILE_ROWS * TILE_ROWS
    tile_end = jnp.cumsum(tile_count)
    tile_start = tile_end - tile_count
    row_pos = tile_start[idx] + sorted_pos - expert_start[idx]
    tile_first = jnp.arange(N_TILES, dtype=jnp.int32) * TILE_ROWS
    tile_expert = jnp.minimum(jnp.sum(tile_end[None, :] <= tile_first[:, None], axis=1, dtype=jnp.int32), N_EXPERTS - 1)
    gy_full = gy.astype(jnp.float32)
    dy_tok = (gate_val[:, None] * gy_full).astype(jnp.bfloat16)
    rows_buf = jnp.zeros((N_TILES * TILE_ROWS, D_MODEL), x.dtype).at[row_pos].set(x)
    dy_buf = jnp.zeros((N_TILES * TILE_ROWS, D_MODEL), dy_tok.dtype).at[row_pos].set(dy_tok)
    grad_init = (jnp.zeros((N_EXPERTS, D_MODEL, D_FF), jnp.float32), jnp.zeros((N_EXPERTS, D_FF, D_MODEL), jnp.float32))
    tiles_in = (rows_buf.reshape(N_TILES, TILE_ROWS, D_MODEL), dy_buf.reshape(N_TILES, TILE_ROWS, D_MODEL), tile_expert)
    grads, tile_out = lax.scan(functools.partial(tile_pass, w_up, w_down), grad_init, tiles_in)
    grad_up, grad_down = grads
    y_tok = tile_out[0].reshape(N_TILES * TILE_ROWS, D_MODEL)[row_pos]
    dx_expert = tile_out[1].reshape(N_TILES * TILE_ROWS, D_MODEL)[row_pos]
    moe_out = (gate_val[:, None] * y_tok.astype(jnp.float32)).astype(jnp.bfloat16)
    d_gate = jnp.sum(gy_full * y_tok.astype(jnp.float32), axis=1)
    d_logit = ((d_gate * gate_val)[:, None] * (onehot.astype(jnp.float32) - router_prob)).astype(jnp.bfloat16)
    dx_router = jnp.dot(d_logit, w_gate.T, preferred_element_type=jnp.float32)
    grad_x = (dx_expert.astype(jnp.float32) + dx_router).astype(jnp.bfloat16)
    grad_gate = jnp.dot(x.T, d_logit, preferred_element_type=jnp.float32)
    return (moe_out, grad_x, grad_up, grad_down, grad_gate)
```

```python
import functools
import jax
import jax.numpy as jnp
from jax import lax
from jax.experimental import pallas as pl
from jax.experimental.pallas import tpu as pltpu
from jax.sharding import PartitionSpec as P


BLK = 16
N_COL = 2
FC = 512
F32 = jnp.float32
BF16 = jnp.bfloat16
GELU_C = 0.7978845608028654
GELU_K = 0.044715
VMEM_LIMIT = 66 * 1000 * 1000


def _any():
    return pl.BlockSpec(memory_space=pl.ANY)


def _smem():
    return pl.BlockSpec(memory_space=pltpu.SMEM)


def _sort_x_kernel(n_exp, rows_buf, idx_ref, x_ref, xs_ref, pos_ref, meta_ref, pos_scr):
    tok = idx_ref.shape[1]
    rows = xs_ref.shape[0]
    step = pl.program_id(0)
    grp = n_exp // N_COL

    @pl.when(step == 0)
    def _():
        col = lax.axis_index('ep') // 2
        exp_iota = lax.broadcasted_iota(jnp.int32, (16, 256), 0)
        tri = (lax.broadcasted_iota(jnp.int32, (256, 256), 0)
               <= lax.broadcasted_iota(jnp.int32, (256, 256), 1)).astype(F32).astype(BF16)
        nchunk = tok // 256
        prefix = []
        carry = jnp.zeros((16, 1), F32)
        for c in range(nchunk):
            oh = (idx_ref[:, c * 256:(c + 1) * 256] == exp_iota).astype(F32).astype(BF16)
            pre = jnp.dot(oh, tri, preferred_element_type=F32)
            prefix.append(pre + (carry - 1.0))
            carry = carry + pre[:, 255:256]
        cnt = carry.astype(jnp.int32)
        nblk = (cnt + (BLK - 1)) >> 4
        start = jnp.zeros((16, 1), jnp.int32)
        iota_col = lax.broadcasted_iota(jnp.int32, (16, 1), 0)
        for g in range(N_COL):
            pre_e = jnp.zeros((1, 1), jnp.int32)
            tot = jnp.zeros((1, 1), jnp.int32)
            for e in range(g * grp, (g + 1) * grp):
                tot = tot + nblk[e:e + 1, :]
            local = (col == g)
            base = jnp.where(local, rows_buf // BLK - tot, 0)
            for e in range(g * grp, (g + 1) * grp):
                start = jnp.where(iota_col == e, base + pre_e, start)
                pre_e = pre_e + nblk[e:e + 1, :]
        lane = lax.broadcasted_iota(jnp.int32, (16, 128), 1)
        meta_ref[...] = jnp.where(lane == 0, start, jnp.where(lane == 1, nblk, 0))
        startf = (start * BLK).astype(F32)
        for c in range(nchunk):
            oh = idx_ref[:, c * 256:(c + 1) * 256] == exp_iota
            p = jnp.sum(jnp.where(oh, prefix[c] + startf, 0.0), axis=0, keepdims=True)
            pos_scr[:, c * 256:(c + 1) * 256] = p.astype(jnp.int32)
        pos_ref[...] = pos_scr[...]

    dst = lax.broadcasted_iota(jnp.int32, (rows, tok), 0) + step * rows
    perm = (dst == pos_scr[...]).astype(F32).astype(BF16)
    xs_ref[...] = jnp.dot(perm, x_ref[...], preferred_element_type=F32).astype(BF16)


def _sort_dy_kernel(n_exp, pos_ref, idxc_ref, x_ref, gy_ref, wg_ref, dys_ref, dy_scr):
    tok = pos_ref.shape[1]
    rows = dys_ref.shape[0]
    step = pl.program_id(0)

    @pl.when(step == 0)
    def _():
        for c in range(tok // 256):
            sl = slice(c * 256, (c + 1) * 256)
            _, _, gate = _router(n_exp, x_ref[sl, :], idxc_ref[sl, :], wg_ref[...])
            dy_scr[sl, :] = (gate * gy_ref[sl, :].astype(F32)).astype(BF16)

    dst = lax.broadcasted_iota(jnp.int32, (rows, tok), 0) + step * rows
    perm = (dst == pos_ref[...]).astype(F32).astype(BF16)
    dys_ref[...] = jnp.dot(perm, dy_scr[...], preferred_element_type=F32).astype(BF16)


def _router(n_exp, x, idx_col, wg):
    lane = lax.broadcasted_iota(jnp.int32, (x.shape[0], wg.shape[1]), 1)
    z = jnp.dot(x, wg, preferred_element_type=F32)
    z = jnp.where(lane < n_exp, z, -jnp.inf)
    ez = jnp.exp(z - jnp.max(z, axis=1, keepdims=True))
    prob = ez / jnp.sum(ez, axis=1, keepdims=True)
    onehot = lane == idx_col
    gate = n_exp * jnp.sum(jnp.where(onehot, prob, 0.0), axis=1, keepdims=True)
    return prob, onehot, gate


def _bits(maxblk):
    b = 1
    while b * 2 <= maxblk:
        b *= 2
    out = []
    while b >= 1:
        out.append(b)
        b //= 2
    return out


def _wait_blocks(n, maxblk, src, dst, sem):
    for b in _bits(maxblk):
        @pl.when((n & b) != 0)
        def _(b=b):
            pltpu.make_async_copy(src.at[pl.ds(0, b * BLK), :], dst.at[pl.ds(0, b * BLK), :], sem).wait()


def _moe_kernel(cfg, *refs):
    n_src, own, acc_in, n_loc, dp_flip, ep_flips, seg_max = cfg
    refs = list(refs)
    meta = refs.pop(0)
    xs = [refs.pop(0) for _ in range(n_src)]
    dys = [refs.pop(0) for _ in range(n_src)]
    w1 = refs.pop(0)
    w2 = refs.pop(0)
    if acc_in:
        g1i = refs.pop(0)
        g2i = refs.pop(0)
    g1o = refs.pop(0)
    g2o = refs.pop(0)
    ys, dxs = [], []
    if own:
        ys = [refs.pop(0) for _ in range(n_src)]
        dxs = [refs.pop(0) for _ in range(n_src)]
    xb = refs.pop(0)
    db = refs.pop(0)
    if own:
        ya = refs.pop(0)
        da_acc = refs.pop(0)
    w1c = refs.pop(0)
    w2c = refs.pop(0)
    a1 = refs.pop(0)
    a2 = refs.pop(0)
    in_sem = refs.pop(0)
    out_sem = refs.pop(0)
    w_sem = refs.pop(0)
    ld_sem = refs.pop(0)
    st_sem = refs.pop(0)

    d_model = w1.shape[1]
    d_ff = w1.shape[2]
    nf = d_ff // FC
    nq = n_loc * nf
    dp = lax.axis_index('dp')
    ep = lax.axis_index('ep')
    n_exp = 4 * n_loc
    seg_bits = _bits(seg_max)

    def seg(e, s):
        sdp = (1 - dp) if dp_flip else dp
        sep = ep ^ ep_flips[s]
        base = ((sdp * 4 + sep) * n_exp + ep * n_loc + e) * 2
        return meta[base], meta[base + 1]

    segs = [[seg(e, s) for s in range(n_src)] for e in range(n_loc)]
    tot = []
    for e in range(n_loc):
        t = segs[e][0][1]
        for s in range(1, n_src):
            t = t + segs[e][s][1]
        tot.append(t)

    def pick(vals, e):
        r = vals[0]
        for i in range(1, n_loc):
            r = jnp.where(e == i, vals[i], r)
        return r

    def seg_loop(e, fn):
        at = jnp.int32(0)
        for s in range(n_src):
            first, num = segs[e][s]
            for b in seg_bits:
                off = num - (num & (2 * b - 1))

                @pl.when((num & b) != 0)
                def _(s=s, b=b, off=off, first=first, at=at):
                    hb = pl.multiple_of((first + off) * BLK, BLK)
                    vb = pl.multiple_of((at + off) * BLK, BLK)
                    fn(s, pl.ds(hb, b * BLK), pl.ds(vb, b * BLK))
            at = at + num

    def w_copies(q):
        e, f, sl = q // nf, q % nf, q % 2
        fo = pl.multiple_of(f * FC, FC)
        return (pltpu.make_async_copy(w1.at[e, :, pl.ds(fo, FC)], w1c.at[sl], w_sem.at[sl, 0]),
                pltpu.make_async_copy(w2.at[e, pl.ds(fo, FC), :], w2c.at[sl], w_sem.at[sl, 1]))

    def ld_copies(q):
        e, f, sl = q // nf, q % nf, q % 3
        fo = pl.multiple_of(f * FC, FC)
        return (pltpu.make_async_copy(g1i.at[e, :, pl.ds(fo, FC)], a1.at[sl], ld_sem.at[sl, 0]),
                pltpu.make_async_copy(g2i.at[e, pl.ds(fo, FC), :], a2.at[sl], ld_sem.at[sl, 1]))

    def st_copies(q):
        e, f, sl = q // nf, q % nf, q % 3
        fo = pl.multiple_of(f * FC, FC)
        return (pltpu.make_async_copy(a1.at[sl], g1o.at[e, :, pl.ds(fo, FC)], st_sem.at[sl, 0]),
                pltpu.make_async_copy(a2.at[sl], g2o.at[e, pl.ds(fo, FC), :], st_sem.at[sl, 1]))

    def start(cs):
        for c in cs:
            c.start()

    def wait(cs):
        for c in cs:
            c.wait()

    start(w_copies(0))
    if acc_in:
        start(ld_copies(0))
    for e in range(n_loc):
        def load(s, hs, vs, e=e):
            pltpu.make_async_copy(xs[s].at[hs, :], xb.at[e, vs, :], in_sem.at[e, 0]).start()
            pltpu.make_async_copy(dys[s].at[hs, :], db.at[e, vs, :], in_sem.at[e, 1]).start()

        seg_loop(e, load)

    def tile(e, r, m, ws, sl):
        r = pl.multiple_of(r, 256)
        x = xb[e, pl.ds(r, m), :]
        dy = db[e, pl.ds(r, m), :]
        a = jnp.dot(x, w1c[ws], preferred_element_type=F32)
        dh = lax.dot_general(dy, w2c[ws], (((1,), (1,)), ((), ())), preferred_element_type=F32)
        a_sq = a * a
        t = jnp.tanh(a * (GELU_C + (GELU_C * GELU_K) * a_sq))
        p = 0.5 + 0.5 * t
        hf = a * p
        gp = p + hf * (1.0 - p) * (2.0 * GELU_C + (6.0 * GELU_C * GELU_K) * a_sq)
        h = hf.astype(BF16)
        da = (gp * dh).astype(BF16)
        if own:
            ya[pl.ds(r, m), :] += jnp.dot(h, w2c[ws], preferred_element_type=F32)
            da_acc[pl.ds(r, m), :] += lax.dot_general(da, w1c[ws], (((1,), (1,)), ((), ())),
                                                      preferred_element_type=F32)
        a2[sl] += lax.dot_general(h, dy, (((0,), (0,)), ((), ())), preferred_element_type=F32)
        a1[sl] += lax.dot_general(x, da, (((0,), (0,)), ((), ())), preferred_element_type=F32)

    def q_step(q, _):
        e, f = q // nf, q % nf
        ws, sl = q % 2, q % 3
        total = pick(tot, e)
        n256 = (total + 15) >> 4

        @pl.when(f == 0)
        def _():
            for s in range(n_src):
                num = pick([segs[i][s][1] for i in range(n_loc)], e)
                _wait_blocks(num, seg_max, xs[0], xb.at[e], in_sem.at[e, 0])
                _wait_blocks(num, seg_max, dys[0], db.at[e], in_sem.at[e, 1])

            def zero_rows(b, _):
                rs = pl.ds(pl.multiple_of(b * BLK, BLK), BLK)
                xb[e, rs, :] = jnp.zeros((BLK, d_model), BF16)
                db[e, rs, :] = jnp.zeros((BLK, d_model), BF16)
                return 0

            lax.fori_loop(total, n256 * 16, zero_rows, 0)
            if own:
                def zero_acc(b, _):
                    rs = pl.ds(pl.multiple_of(b * 256, 256), 256)
                    ya[rs, :] = jnp.zeros((256, d_model), F32)
                    da_acc[rs, :] = jnp.zeros((256, d_model), F32)
                    return 0

                lax.fori_loop(0, n256, zero_acc, 0)

        if acc_in:
            @pl.when(q + 1 < nq)
            def _():
                @pl.when(q >= 2)
                def _():
                    wait(st_copies(q - 2))

                start(ld_copies(q + 1))

            wait(ld_copies(q))
        else:
            @pl.when(q >= 3)
            def _():
                wait(st_copies(q - 3))

            a1[sl] = jnp.zeros(a1.shape[1:], F32)
            a2[sl] = jnp.zeros(a2.shape[1:], F32)
        wait(w_copies(q))

        @pl.when(q + 1 < nq)
        def _():
            start(w_copies(q + 1))

        n512 = n256 >> 1
        lax.fori_loop(0, n512, lambda i, _: (tile(e, i * 512, 512, ws, sl), 0)[1], 0)

        @pl.when((n256 & 1) == 1)
        def _():
            tile(e, n512 * 512, 256, ws, sl)

        start(st_copies(q))

        if own:
            @pl.when(f == nf - 1)
            def _():
                def cast(b, _):
                    rs = pl.ds(pl.multiple_of(b * 256, 256), 256)
                    xb[e, rs, :] = ya[rs, :].astype(BF16)
                    db[e, rs, :] = da_acc[rs, :].astype(BF16)
                    return 0

                lax.fori_loop(0, n256, cast, 0)
                for i in range(n_loc):
                    @pl.when(e == i)
                    def _(i=i):
                        def put(s, hs, vs):
                            pltpu.make_async_copy(xb.at[i, vs, :], ys[s].at[hs, :], out_sem.at[i, 0]).start()
                            pltpu.make_async_copy(db.at[i, vs, :], dxs[s].at[hs, :], out_sem.at[i, 1]).start()

                        seg_loop(i, put)
        return 0

    lax.fori_loop(0, nq, q_step, 0)
    for q in range(nq - 3, nq):
        wait(st_copies(q))
    if own:
        for i in range(n_loc):
            for s in range(n_src):
                _wait_blocks(segs[i][s][1], seg_max, xb.at[i], ys[0], out_sem.at[i, 0])
                _wait_blocks(segs[i][s][1], seg_max, db.at[i], dxs[0], out_sem.at[i, 1])


def _moe_call(meta, xs, dys, w1, w2, own, acc, dp_flip, ep_flips, seg_max, flops):
    n_src = len(xs)
    n_loc, d_model, _ = w1.shape
    cap = n_src * seg_max * BLK
    g_shapes = [jax.ShapeDtypeStruct(w1.shape, F32), jax.ShapeDtypeStruct(w2.shape, F32)]
    outs = list(g_shapes)
    if own:
        outs += [jax.ShapeDtypeStruct(a.shape, BF16) for a in xs] * 2
    scratch = [pltpu.VMEM((n_loc, cap, d_model), BF16)] * 2
    if own:
        scratch += [pltpu.VMEM((cap, d_model), F32)] * 2
    scratch += [
        pltpu.VMEM((2, d_model, FC), BF16), pltpu.VMEM((2, FC, d_model), BF16),
        pltpu.VMEM((3, d_model, FC), F32), pltpu.VMEM((3, FC, d_model), F32),
        pltpu.SemaphoreType.DMA((n_loc, 2)), pltpu.SemaphoreType.DMA((n_loc, 2)),
        pltpu.SemaphoreType.DMA((2, 2)), pltpu.SemaphoreType.DMA((3, 2)), pltpu.SemaphoreType.DMA((3, 2)),
    ]
    args = [meta, *xs, *dys, w1, w2]
    aliases = {}
    if acc is not None:
        aliases = {len(args): 0, len(args) + 1: 1}
        args += list(acc)
    cfg = (n_src, own, acc is not None, n_loc, dp_flip, ep_flips, seg_max)
    return pl.pallas_call(
        functools.partial(_moe_kernel, cfg),
        out_shape=outs,
        in_specs=[_smem()] + [_any()] * (len(args) - 1),
        out_specs=[_any()] * len(outs),
        scratch_shapes=scratch,
        input_output_aliases=aliases,
        compiler_params=pltpu.CompilerParams(vmem_limit_bytes=VMEM_LIMIT),
        cost_estimate=pl.CostEstimate(flops=flops, bytes_accessed=60_000_000, transcendentals=0),
    )(*args)


def _merge(bounds, far_ref, mine_ref, pair_ref, dst_ref):
    rows = dst_ref.shape[0]
    pre_end, suf_start, split, mine_first = bounds[0], bounds[1], bounds[2], bounds[3]
    step = 272
    for c in range(rows // step):
        row = lax.broadcasted_iota(jnp.int32, (step, 1), 0) + c * step
        sl = slice(c * step, (c + 1) * step)
        first = row < split
        take_mine = first == (mine_first == 1)
        loc = jnp.where(take_mine, mine_ref[sl, :].astype(F32), pair_ref[sl, :].astype(F32))
        far = far_ref[sl, :].astype(F32)
        v = jnp.where(row < pre_end, far, jnp.where(row >= suf_start, loc, 0.0))
        dst_ref[sl, :] = v.astype(BF16)


def _fin_y_kernel(n_exp, bounds, far_ref, mine_ref, pair_ref, posc_ref, idxc_ref, x_ref, gy_ref, wg_ref,
                  out_ref, dz_ref, dwg_ref, y_scr):
    step = pl.program_id(0)

    @pl.when(step == 0)
    def _():
        _merge(bounds, far_ref, mine_ref, pair_ref, y_scr)
        dwg_ref[...] = jnp.zeros_like(dwg_ref)

    m = posc_ref.shape[0]
    sel = (lax.broadcasted_iota(jnp.int32, (m, y_scr.shape[0]), 1) == posc_ref[...]).astype(F32).astype(BF16)
    y = jnp.dot(sel, y_scr[...], preferred_element_type=F32)
    prob, onehot, gate = _router(n_exp, x_ref[...], idxc_ref[...], wg_ref[...])
    out_ref[...] = (gate * y).astype(BF16)
    d_gate = jnp.sum(gy_ref[...].astype(F32) * y, axis=1, keepdims=True)
    dz = ((d_gate * gate) * (onehot.astype(F32) - prob)).astype(BF16)
    dz_ref[...] = dz
    dwg_ref[...] += lax.dot_general(x_ref[...], dz, (((0,), (0,)), ((), ())), preferred_element_type=F32)


def _fin_dx_kernel(bounds, far_ref, mine_ref, pair_ref, posc_ref, dz_ref, wg_ref, dx_ref, scr):
    step = pl.program_id(0)

    @pl.when(step == 0)
    def _():
        _merge(bounds, far_ref, mine_ref, pair_ref, scr)

    m = posc_ref.shape[0]
    sel = (lax.broadcasted_iota(jnp.int32, (m, scr.shape[0]), 1) == posc_ref[...]).astype(F32).astype(BF16)
    dxe = jnp.dot(sel, scr[...], preferred_element_type=F32)
    dxr = lax.dot_general(dz_ref[...], wg_ref[...], (((1,), (1,)), ((), ())), preferred_element_type=F32)
    dx_ref[...] = (dxe + dxr).astype(BF16)


def solution(mesh):
    tok_spec = P(('dp', 'ep'), None)
    idx_spec = P(('dp', 'ep'))
    rep_spec = P(None, None)
    exp_spec = P('ep', None, None)
    ep_size = mesh.shape['ep']
    dp_size = mesh.shape['dp']
    n_dev = ep_size * dp_size

    def local_step(x, gy, idx, w_gate, w_up, w_down):
        tok, d_model = x.shape
        n_exp = w_gate.shape[1]
        seg_max = (tok // 2) // BLK
        rows_buf = tok + 128
        ep = lax.axis_index('ep')
        dp = lax.axis_index('dp')
        col = ep // 2
        vm = pltpu.CompilerParams(vmem_limit_bytes=VMEM_LIMIT)
        wg_pad = jnp.pad(w_gate, ((0, 0), (0, 128 - n_exp)))
        idx_row = idx.reshape(1, tok)
        idx_col = idx.reshape(tok, 1)

        def whole(shape):
            return pl.BlockSpec(shape, lambda i: (0,) * len(shape))

        def const_smem():
            return pl.BlockSpec(memory_space=pltpu.SMEM)

        st = rows_buf // 4
        xs, pos, meta = pl.pallas_call(
            functools.partial(_sort_x_kernel, n_exp, rows_buf),
            grid=(4,),
            out_shape=[jax.ShapeDtypeStruct((rows_buf, d_model), BF16),
                       jax.ShapeDtypeStruct((1, tok), jnp.int32),
                       jax.ShapeDtypeStruct((16, 128), jnp.int32)],
            in_specs=[whole((1, tok)), whole((tok, d_model))],
            out_specs=[pl.BlockSpec((st, d_model), lambda i: (i, 0)), whole((1, tok)), whole((16, 128))],
            scratch_shapes=[pltpu.VMEM((1, tok), jnp.int32)],
            compiler_params=vm,
            cost_estimate=pl.CostEstimate(flops=7_000_000_000, bytes_accessed=8_000_000, transcendentals=0),
            name='sort_x',
        )(idx_row, x)
        dys = pl.pallas_call(
            functools.partial(_sort_dy_kernel, n_exp),
            grid=(4,),
            out_shape=jax.ShapeDtypeStruct((rows_buf, d_model), BF16),
            in_specs=[whole((1, tok)), whole((tok, 1)), whole((tok, d_model)), whole((tok, d_model)),
                      whole((d_model, 128))],
            out_specs=pl.BlockSpec((st, d_model), lambda i: (i, 0)),
            scratch_shapes=[pltpu.VMEM((tok, d_model), BF16)],
            compiler_params=vm,
            cost_estimate=pl.CostEstimate(flops=8_000_000_000, bytes_accessed=12_000_000, transcendentals=0),
            name='sort_dy',
        )(pos, idx_col, x, gy, wg_pad)

        meta_loc = meta[:n_exp, :2].reshape(1, n_exp * 2)
        meta_all = lax.all_gather(meta_loc, ('dp', 'ep'), axis=0, tiled=True)
        meta_flat = meta_all.reshape(n_dev * n_exp * 2)

        def pair(a):
            return lax.ppermute(a, 'ep', [(i, i ^ 1) for i in range(ep_size)])

        def cross_x(a):
            return lax.ppermute(a, 'ep', [(i, i ^ 2) for i in range(ep_size)])

        def cross_y(a):
            return lax.ppermute(a, 'dp', [(i, 1 - i) for i in range(dp_size)])

        def moe(*args):
            return _moe_call(meta_flat, *args)

        xs_d = pair(xs)
        xs_x = cross_x(xs)
        xs_y = cross_y(xs)
        dys_d = pair(dys)
        dys_x = cross_x(dys)
        dys_y = cross_y(dys)

        g1, g2, y_0, y_d, dx_0, dx_d = moe(
            [xs, xs_d], [dys, dys_d], w_up, w_down, True, None, False, (0, 1), seg_max, 45_000_000_000)
        xs_xd = pair(xs_x)
        dys_xd = pair(dys_x)
        xs_g = cross_y(xs_x)
        dys_g = cross_y(dys_x)
        xs_yd = pair(xs_y)
        dys_yd = pair(dys_y)
        y_dr = pair(y_d)
        dx_dr = pair(dx_d)
        g1, g2, y_x, y_xd, dx_x, dx_xd = moe(
            [xs_x, xs_xd], [dys_x, dys_xd], w_up, w_down, True, (g1, g2), False, (2, 3), seg_max,
            45_000_000_000)

        meta_t = meta_all.reshape(dp_size, ep_size, n_exp, 2)
        grp = n_exp // N_COL
        m_far = lax.dynamic_slice(meta_t, (dp, ep ^ 2, grp * col + grp // 2, 0), (1, 1, 1, 1)).reshape(())
        row = lax.broadcasted_iota(jnp.int32, (rows_buf, 1), 0)
        take = (row < m_far * BLK) == ((ep % 2) == 0)
        y_m = jnp.where(take, y_x, pair(y_xd))
        dx_m = jnp.where(take, dx_x, pair(dx_xd))
        y_ret = cross_x(y_m)
        dx_ret = cross_x(dx_m)

        g1, g2 = moe(
            [xs_y, xs_yd], [dys_y, dys_yd], w_up, w_down, False, (g1, g2), True, (0, 1), seg_max,
            30_000_000_000)
        xs_gd = pair(xs_g)
        dys_gd = pair(dys_g)
        g1, g2 = moe(
            [xs_g, xs_gd], [dys_g, dys_gd], w_up, w_down, False, (g1, g2), True, (2, 3), seg_max,
            30_000_000_000)

        mine = lax.dynamic_slice(meta_t, (dp, ep, 0, 0), (1, 1, n_exp, 2)).reshape(n_exp, 2)
        far_last = lax.dynamic_slice(mine, (grp * (1 - col) + grp - 1, 0), (1, 2)).reshape(2)
        near = lax.dynamic_slice(mine, (grp * col, 0), (grp, 2))
        b_iota = lax.broadcasted_iota(jnp.int32, (4,), 0)
        bounds = jnp.where(b_iota == 0, (far_last[0] + far_last[1]) * BLK,
                           jnp.where(b_iota == 1, near[0, 0] * BLK,
                                     jnp.where(b_iota == 2, near[grp // 2, 0] * BLK, 1 - ep % 2)))
        pos_col = pos.reshape(tok, 1)
        tm = 256

        def rows_spec(width):
            return pl.BlockSpec((tm, width), lambda i: (i, 0))

        moe_out, dz, dwg = pl.pallas_call(
            functools.partial(_fin_y_kernel, n_exp),
            grid=(tok // tm,),
            out_shape=[jax.ShapeDtypeStruct((tok, d_model), BF16), jax.ShapeDtypeStruct((tok, 128), BF16),
                       jax.ShapeDtypeStruct((d_model, 128), F32)],
            in_specs=[const_smem()] + [whole((rows_buf, d_model))] * 3 + [
                rows_spec(1), rows_spec(1), rows_spec(d_model), rows_spec(d_model), whole((d_model, 128))],
            out_specs=[rows_spec(d_model), rows_spec(128), whole((d_model, 128))],
            scratch_shapes=[pltpu.VMEM((rows_buf, d_model), BF16)],
            compiler_params=vm,
            cost_estimate=pl.CostEstimate(flops=8_000_000_000, bytes_accessed=20_000_000, transcendentals=0),
            name='fin_y',
        )(bounds, y_ret, y_0, y_dr, pos_col, idx_col, x, gy, wg_pad)
        grad_gate = lax.psum(dwg[:, :n_exp], ('dp', 'ep'))
        grad_x = pl.pallas_call(
            _fin_dx_kernel,
            grid=(tok // tm,),
            out_shape=jax.ShapeDtypeStruct((tok, d_model), BF16),
            in_specs=[const_smem()] + [whole((rows_buf, d_model))] * 3 + [
                rows_spec(1), rows_spec(128), whole((d_model, 128))],
            out_specs=rows_spec(d_model),
            scratch_shapes=[pltpu.VMEM((rows_buf, d_model), BF16)],
            compiler_params=vm,
            cost_estimate=pl.CostEstimate(flops=8_000_000_000, bytes_accessed=20_000_000, transcendentals=0),
            name='fin_dx',
        )(bounds, dx_ret, dx_0, dx_dr, pos_col, dz, wg_pad)
        return moe_out, grad_x, g1, g2, grad_gate

    return jax.shard_map(local_step, mesh=mesh,
                         in_specs=(tok_spec, tok_spec, idx_spec, rep_spec, exp_spec, exp_spec),
                         out_specs=(tok_spec, tok_spec, exp_spec, exp_spec, rep_spec), check_vma=False)
```
